32 devices in a mesh: row: 4 (over y, core), col: 4 (over z), layer: 2 (over x).
Axes of the slice: x: 2, y: 2, z: 4, core: 2. Of those that a mesh axis runs over, the one named last changes fastest.
Arguments:
- hamiltonian: bfloat16 [2560, 2560], P(('row', 'layer'), 'col'), may hold values from -1.2 to 1.2, as said below
- tile_pattern: int32 [20, 20], replicated, may hold values from 0 to 1, as said below
- n_occ: int32 [1], replicated, may hold values from 512 to 2047
- mu: float32 [1], replicated, may hold values from -0.2 to 0.2
- gamma: float32 [1], replicated, may hold values from 0.25 to 0.4
Outputs:
- density: float32 [2560, 2560], P(('row', 'layer'), 'col')
The draws below stay inside these ranges and needn't reach their ends.
Inputs may be any that keep to these rules, and one draw needn't show every extreme that they name: `tile_pattern`: Symmetric, 0 or 1, with ones on the diagonal and next to it. `hamiltonian`: Symmetric; its eigenvalues lie within -1.8 and 1.8.
All inputs are finite; a program needn't handle non-finite values.
Results may differ from the reference program's by a relative error of at most 0.0055.
Values may be sent and summed in bfloat16 or wider, within the bound.
A program may use at most 64 MiB of HBM per device.

```python
import jax
import jax.numpy as jnp

TILE = 128
STEPS = 2
TILES = 20
NORB = 2560


def tile_layout(key):
    row_ids = jnp.arange(TILES, dtype=jnp.int32)[:, None]
    col_ids = jnp.arange(TILES, dtype=jnp.int32)[None, :]
    tile_score = jax.random.randint(key, (TILES, TILES), 0, 100, dtype=jnp.int32)
    tile_score = jnp.where(row_ids <= col_ids, tile_score, tile_score.T)
    chance = 3 + 30 * (row_ids + col_ids) // (2 * TILES)
    near_diag = jnp.abs(row_ids - col_ids) <= 1
    return jnp.where(near_diag | (tile_score < chance), 1, 0).astype(jnp.int32)


def draw_tile_pattern(key, part):
    return tile_layout(jax.random.fold_in(key, 7))


def draw_hamiltonian(key, part):
    pattern = tile_layout(jax.random.fold_in(key, 7))
    dense_mask = jnp.repeat(jnp.repeat(pattern, TILE, 0), TILE, 1).astype(jnp.float32)
    row_count = jnp.sum(dense_mask, axis=1)
    row_weight = row_count ** (-0.25)
    first_key, second_key = jax.random.split(jax.random.fold_in(key, 13))
    noise_field = jax.random.normal(first_key, (NORB, NORB), jnp.float32)
    onsite = jax.random.uniform(second_key, (NORB,), jnp.float32, -0.2, 0.2)
    noise_field = jnp.clip((noise_field + noise_field.T) * 0.7071, -4.0, 4.0)
    identity = jnp.eye(NORB, dtype=jnp.float32)
    scaling = 0.65 * row_weight[:, None] * row_weight[None, :]
    coupled = dense_mask * scaling * noise_field * (1.0 - identity)
    return (coupled + identity * onsite[None, :]).astype(jnp.bfloat16)


def setup_inputs(seed: int = 0) -> dict:
    streams_of = jax.random.split(jax.random.key(seed), 6)
    hamiltonian = draw_hamiltonian(jax.random.fold_in(streams_of[5], 71), 0)
    tile_pattern = draw_tile_pattern(jax.random.fold_in(streams_of[5], 71), 0)
    n_occ = jax.random.randint(streams_of[2], (1,), NORB // 5, 4 * NORB // 5).astype(jnp.int32)
    mu = jnp.clip(jax.random.uniform(streams_of[3], (1,), jnp.float32, -0.2, 0.2), -0.2, 0.2)
    gamma = jnp.clip(jax.random.uniform(streams_of[4], (1,), jnp.float32, 0.25, 0.4), 0.25, 0.4)
    return dict(hamiltonian=hamiltonian, tile_pattern=tile_pattern, n_occ=n_occ, mu=mu, gamma=gamma)


def reference(hamiltonian, tile_pattern, n_occ, mu, gamma):
    mask = jnp.repeat(jnp.repeat(tile_pattern, TILE, 0), TILE, 1).astype(jnp.float32)
    identity = jnp.eye(NORB, dtype=jnp.float32)
    filling = n_occ[0].astype(jnp.float32) / NORB
    start = mask * (filling * identity + gamma[0] * (mu[0] * identity - hamiltonian.astype(jnp.float32)))
    current = start.astype(jnp.bfloat16)
    result = start
    for iteration in range(STEPS):
        square = mask * jnp.dot(current, current, preferred_element_type=jnp.float32)
        cube = mask * jnp.dot(square.astype(jnp.bfloat16), current, preferred_element_type=jnp.float32)
        result = 3.0 * square - 2.0 * cube
        current = result.astype(jnp.bfloat16)
    return result
```

```python
import functools

import jax
import jax.numpy as jnp
from jax import lax
from jax.experimental import pallas as pl
from jax.experimental.pallas import tpu as pltpu
from jax.sharding import PartitionSpec as P

TILE = 128
STEPS = 2


def element_mask(tile_pattern, row_start, row_count, col_start, col_count):
    tile_count = tile_pattern.shape[0]
    tile_ids = jnp.arange(tile_count, dtype=jnp.int32)
    row_tiles = (row_start + jnp.arange(row_count, dtype=jnp.int32)) // TILE
    col_tiles = (col_start + jnp.arange(col_count, dtype=jnp.int32)) // TILE
    row_hot = (row_tiles[:, None] == tile_ids[None, :]).astype(jnp.bfloat16)
    col_hot = (tile_ids[:, None] == col_tiles[None, :]).astype(jnp.bfloat16)
    picked = jnp.dot(row_hot, tile_pattern.astype(jnp.bfloat16), preferred_element_type=jnp.float32)
    return jnp.dot(picked.astype(jnp.bfloat16), col_hot, preferred_element_type=jnp.float32)


def plain_shards(hamiltonian, tile_pattern, n_occ, mu, gamma):
    share_rows, band_cols = hamiltonian.shape
    n_col = lax.axis_size("col")
    n_layer = lax.axis_size("layer")
    order = band_cols * n_col
    layer_index = lax.axis_index("layer")
    row_start = (lax.axis_index("row") * n_layer + layer_index) * share_rows
    col_start = lax.axis_index("col") * band_cols
    mask = element_mask(tile_pattern, row_start, share_rows, col_start, band_cols)
    row_global = row_start + jnp.arange(share_rows, dtype=jnp.int32)
    col_global = col_start + jnp.arange(band_cols, dtype=jnp.int32)
    identity = (row_global[:, None] == col_global[None, :]).astype(jnp.float32)
    filling = n_occ[0].astype(jnp.float32) / order
    start = mask * (
        filling * identity + gamma[0] * (mu[0] * identity - hamiltonian.astype(jnp.float32))
    )
    current = start.astype(jnp.bfloat16)
    result = start
    for iteration in range(STEPS):
        column = lax.all_gather(current, ("row", "layer"), axis=0, tiled=True)

        def rows_product(left_share):
            return jnp.dot(
                lax.all_gather(left_share, "col", axis=1, tiled=True),
                column,
                preferred_element_type=jnp.float32,
            )

        square = mask * rows_product(current)
        cube = mask * rows_product(square.astype(jnp.bfloat16))
        result = 3.0 * square - 2.0 * cube
        current = result.astype(jnp.bfloat16)
    return result


F32 = jnp.float32
BF16 = jnp.bfloat16
Z_UP, Z_DOWN, L_UP, L_DOWN, TO_Y, TO_CORE = range(6)


def kernel(sizes, cur, flags, out, full, square, half, half2, strip, column, send1, recv1, send2, recv2, send3, recv3):
    n_row, n_col, n_layer, bm, bn = sizes
    order = bn * n_col
    half_order = order // 2
    bands = n_col // 2
    row, z, layer = lax.axis_index("row"), lax.axis_index("col"), lax.axis_index("layer")
    y, core = row // 2, row % 2
    row_y = (1 - y) * 2 + core
    row_c = y * 2 + 1 - core
    row_yc = (1 - y) * 2 + 1 - core

    barrier = pltpu.get_barrier_semaphore()

    def greet(cond, device):
        @pl.when(cond)
        def _():
            pl.semaphore_signal(barrier, inc=1, device_id=device, device_id_type=pl.DeviceIdType.MESH)

    neighbours = [
        (z > 0, {"col": z - 1}),
        (z < n_col - 1, {"col": z + 1}),
        (layer > 0, {"layer": layer - 1}),
        (layer < n_layer - 1, {"layer": layer + 1}),
    ]
    for cond, device in neighbours:
        greet(cond, device)
    for device in ({"row": row_y}, {"row": row_c}):
        pl.semaphore_signal(barrier, inc=1, device_id=device, device_id_type=pl.DeviceIdType.MESH)
    peers = 2
    for cond, _device in neighbours:
        peers = peers + jnp.where(cond, 1, 0)
    pl.semaphore_wait(barrier, peers)

    def rows_of(r, l):
        return pl.ds(pl.multiple_of((r * n_layer + l) * bm, bm), bm)

    def cols_of(b):
        return pl.ds(pl.multiple_of(b * bn, bn), bn)

    def always(cond, body):
        if cond is None:
            body()
        else:
            pl.when(cond)(body)

    def both(a, b):
        if a is None:
            return b
        if b is None:
            return a
        return jnp.logical_and(a, b)

    class Gather:
        def __init__(self, view, index, send, recv):
            self.view, self.index, self.send, self.recv = view, index, send, recv
            self.pending = []

        def copy(self, way, block, device, src=None):
            dst = self.view(*block)
            at = self.index(*block)
            return pltpu.make_async_remote_copy(
                src_ref=dst if src is None else src,
                dst_ref=dst,
                send_sem=self.send.at[way, at],
                recv_sem=self.recv.at[at],
                device_id=device,
                device_id_type=pl.DeviceIdType.MESH,
            )

        def start(self, cond, way, block, device, src=None):
            always(cond, lambda: self.copy(way, block, device, src).start())
            self.pending.append((cond, way, block, device, src))

        def arrive(self, cond, block):
            always(cond, lambda: self.copy(TO_CORE, block, {"row": row_c}).wait_recv())

        def drain(self):
            for cond, way, block, device, src in self.pending:
                always(cond, lambda: self.copy(way, block, device, src).wait_send())

    g = Gather(
        lambda r, l, b: full.at[rows_of(r, l), cols_of(b)],
        lambda r, l, b: (r * n_layer + l) * n_col + b,
        send1,
        recv1,
    )

    def spread(cond, block, up, down, src=None):
        r, l, b = block
        if up:
            g.start(both(cond, layer < n_layer - 1), L_UP, block, {"layer": layer + 1}, src)
        if down:
            g.start(both(cond, layer > 0), L_DOWN, block, {"layer": layer - 1}, src)
        g.start(both(cond, b // bands == y), TO_Y, block, {"row": row_y}, src)
        g.start(cond, TO_CORE, block, {"row": row_c}, src)

    mine = (row, layer, z)
    g.start(z < n_col - 1, Z_UP, mine, {"col": z + 1}, cur)
    g.start(z > 0, Z_DOWN, mine, {"col": z - 1}, cur)
    spread(None, mine, True, True, cur)
    full[rows_of(row, layer), cols_of(z)] = cur[...]

    def layer_arrivals(cond, b):
        for e in range(1, n_layer):
            for sign in (-1, 1):
                l = layer + sign * e
                inside = both(cond, l >= 0 if sign < 0 else l < n_layer)
                g.arrive(inside, (row, l, b))
                spread(inside, (row, l, b), sign < 0, sign > 0)

    for d in range(1, n_col):
        for sign in (-1, 1):
            b = z + sign * d
            inside = b >= 0 if sign < 0 else b < n_col
            block = (row, layer, b)
            g.arrive(inside, block)
            if sign < 0:
                g.start(both(inside, z < n_col - 1), Z_UP, block, {"col": z + 1})
            else:
                g.start(both(inside, z > 0), Z_DOWN, block, {"col": z - 1})
            spread(inside, block, True, True)
        if d == 1:
            layer_arrivals(None, z)
        else:
            layer_arrivals(z - d + 1 >= 0, z - d + 1)
            layer_arrivals(z + d - 1 < n_col, z + d - 1)
    layer_arrivals(z - n_col + 1 >= 0, z - n_col + 1)
    layer_arrivals(z + n_col - 1 < n_col, z + n_col - 1)
    for b in range(bands):
        for l in range(n_layer):
            block = (row_y, l, (1 - y) * bands + b)
            g.arrive(None, block)
            g.start(None, TO_CORE, block, {"row": row_c})
    for l in range(n_layer):
        for b in range(n_col):
            g.arrive(None, (row_c, l, b))
        for b in range(bands):
            g.arrive(None, (row_yc, l, (1 - y) * bands + b))
    g.drain()

    mine_at = pl.multiple_of(y * half_order, half_order)
    other_at = pl.multiple_of((1 - y) * half_order, half_order)

    @pl.loop(0, half_order // TILE)
    def _(t):
        here = pl.ds(pl.multiple_of(mine_at + t * TILE, TILE), TILE)
        full[pl.ds(other_at, half_order), here] = full[here, pl.ds(other_at, half_order)].T

    own_rows = rows_of(row, layer)

    def mask_of(b):
        tiles = flags.shape[1]
        tile = lax.broadcasted_iota(jnp.int32, (tiles, bn), 0)
        column_tile = (b * bn + lax.broadcasted_iota(jnp.int32, (tiles, bn), 1)) // TILE
        return jnp.dot(flags[...], (tile == column_tile).astype(BF16), preferred_element_type=F32)

    @pl.loop(0, n_col)
    def _(b):
        value = mask_of(b) * jnp.dot(full[own_rows, :], full[:, cols_of(b)], preferred_element_type=F32)
        square[:, cols_of(b)] = value
        half[:, cols_of(b)] = value.astype(BF16)

    c = Gather(
        lambda r, l: column.at[rows_of(r, l), :],
        lambda r, l: r * n_layer + l,
        send2,
        recv2,
    )

    def cube_band(b):
        cube = mask_of(b) * jnp.dot(half[...], full[:, cols_of(b)], preferred_element_type=F32)
        return (3.0 * square[:, cols_of(b)] - 2.0 * cube).astype(BF16)

    def spread_column(cond, block, up, down):
        if up:
            c.start(both(cond, layer < n_layer - 1), L_UP, block, {"layer": layer + 1})
        if down:
            c.start(both(cond, layer > 0), L_DOWN, block, {"layer": layer - 1})
        c.start(cond, TO_Y, block, {"row": row_y})
        c.start(cond, TO_CORE, block, {"row": row_c})

    first = cube_band(z)
    column[own_rows, :] = first
    strip[:, cols_of(z)] = first
    spread_column(None, (row, layer), True, True)

    @pl.loop(1, n_col)
    def _(i):
        b = lax.rem(z + i, n_col)
        strip[:, cols_of(b)] = cube_band(b)

    for e in range(1, n_layer):
        for sign in (-1, 1):
            l = layer + sign * e
            inside = l >= 0 if sign < 0 else l < n_layer
            c.arrive(inside, (row, l))
            spread_column(inside, (row, l), sign < 0, sign > 0)
    for l in range(n_layer):
        c.arrive(None, (row_y, l))
        c.start(None, TO_CORE, (row_y, l), {"row": row_c})
    for l in range(n_layer):
        c.arrive(None, (row_c, l))
    for l in range(n_layer):
        c.arrive(None, (row_yc, l))

    mask_z = mask_of(z)
    last = mask_z * jnp.dot(strip[...], column[...], preferred_element_type=F32)
    out[...] = 3.0 * last
    half2[:, cols_of(z)] = last.astype(BF16)
    s = Gather(lambda b: half2.at[:, cols_of(b)], lambda b: b, send3, recv3)
    s.start(z < n_col - 1, Z_UP, (z,), {"col": z + 1})
    s.start(z > 0, Z_DOWN, (z,), {"col": z - 1})

    def cube_part(b):
        part = jnp.dot(half2[:, cols_of(b)], column[cols_of(b), :], preferred_element_type=F32)
        out[...] -= (2.0 * mask_z) * part

    cube_part(z)
    for d in range(1, n_col):
        for sign in (-1, 1):
            b = z + sign * d
            inside = b >= 0 if sign < 0 else b < n_col
            s.arrive(inside, (b,))
            if sign < 0:
                s.start(both(inside, z < n_col - 1), Z_UP, (b,), {"col": z + 1})
            else:
                s.start(both(inside, z > 0), Z_DOWN, (b,), {"col": z - 1})
        for sign in (-1, 1):
            b = z + sign * d
            inside = b >= 0 if sign < 0 else b < n_col
            always(inside, functools.partial(cube_part, b))
    s.drain()
    c.drain()


def shards(hamiltonian, tile_pattern, n_occ, mu, gamma):
    bm, bn = hamiltonian.shape
    n_row, n_col, n_layer = (lax.axis_size(a) for a in ("row", "col", "layer"))
    order = bn * n_col
    vmem = 2 * order * (order + 3 * bm + bn) + 4 * bm * (order + bn) + 2 * bm * bn
    regular = n_row == 4 and n_col % 2 == 0 and n_layer * bm * n_row == order
    aligned = bm % 16 == 0 and bn % TILE == 0 and (order // 2) % TILE == 0
    if not (regular and aligned and vmem <= 48 << 20):
        return plain_shards(hamiltonian, tile_pattern, n_occ, mu, gamma)
    row_start = (lax.axis_index("row") * n_layer + lax.axis_index("layer")) * bm
    col_start = lax.axis_index("col") * bn
    rows = row_start + jnp.arange(bm, dtype=jnp.int32)
    cols = col_start + jnp.arange(bn, dtype=jnp.int32)
    tile_ids = jnp.arange(tile_pattern.shape[0], dtype=jnp.int32)
    row_hot = (rows[:, None] // TILE == tile_ids[None, :]).astype(BF16)
    flags = jnp.dot(row_hot, tile_pattern.astype(BF16), preferred_element_type=F32).astype(BF16)
    col_hot = (tile_ids[:, None] == cols[None, :] // TILE).astype(BF16)
    mask = jnp.dot(flags, col_hot, preferred_element_type=F32)
    identity = (rows[:, None] == cols[None, :]).astype(F32)
    filling = n_occ[0].astype(F32) / order
    start = mask * (filling * identity + gamma[0] * (mu[0] * identity - hamiltonian.astype(F32)))
    blocks = n_row * n_layer
    return pl.pallas_call(
        functools.partial(kernel, (n_row, n_col, n_layer, bm, bn)),
        out_shape=jax.ShapeDtypeStruct((bm, bn), F32),
        in_specs=[pl.BlockSpec(memory_space=pltpu.VMEM)] * 2,
        out_specs=pl.BlockSpec(memory_space=pltpu.VMEM),
        scratch_shapes=[
            pltpu.VMEM((order, order), BF16),
            pltpu.VMEM((bm, order), F32),
            pltpu.VMEM((bm, order), BF16),
            pltpu.VMEM((bm, order), BF16),
            pltpu.VMEM((bm, order), BF16),
            pltpu.VMEM((order, bn), BF16),
            pltpu.SemaphoreType.DMA((6, blocks * n_col)),
            pltpu.SemaphoreType.DMA((blocks * n_col,)),
            pltpu.SemaphoreType.DMA((6, blocks)),
            pltpu.SemaphoreType.DMA((blocks,)),
            pltpu.SemaphoreType.DMA((2, n_col)),
            pltpu.SemaphoreType.DMA((n_col,)),
        ],
        compiler_params=pltpu.CompilerParams(
            collective_id=0, has_side_effects=True, vmem_limit_bytes=60 << 20
        ),
    )(start.astype(BF16), flags)


def solution(mesh):
    placed = (P(("row", "layer"), "col"), P(), P(), P(), P())
    return jax.shard_map(
        shards, mesh=mesh, in_specs=placed, out_specs=P(("row", "layer"), "col"), check_vma=False
    )
```

```python
import functools

import jax
import jax.numpy as jnp
from jax import lax
from jax.experimental import pallas as pl
from jax.experimental.pallas import tpu as pltpu
from jax.sharding import PartitionSpec as P

TILE = 128
STEPS = 2


def element_mask(tile_pattern, row_start, row_count, col_start, col_count):
    tile_count = tile_pattern.shape[0]
    tile_ids = jnp.arange(tile_count, dtype=jnp.int32)
    row_tiles = (row_start + jnp.arange(row_count, dtype=jnp.int32)) // TILE
    col_tiles = (col_start + jnp.arange(col_count, dtype=jnp.int32)) // TILE
    row_hot = (row_tiles[:, None] == tile_ids[None, :]).astype(jnp.bfloat16)
    col_hot = (tile_ids[:, None] == col_tiles[None, :]).astype(jnp.bfloat16)
    picked = jnp.dot(row_hot, tile_pattern.astype(jnp.bfloat16), preferred_element_type=jnp.float32)
    return jnp.dot(picked.astype(jnp.bfloat16), col_hot, preferred_element_type=jnp.float32)


def plain_shards(hamiltonian, tile_pattern, n_occ, mu, gamma):
    share_rows, band_cols = hamiltonian.shape
    n_col = lax.axis_size("col")
    n_layer = lax.axis_size("layer")
    order = band_cols * n_col
    layer_index = lax.axis_index("layer")
    row_start = (lax.axis_index("row") * n_layer + layer_index) * share_rows
    col_start = lax.axis_index("col") * band_cols
    mask = element_mask(tile_pattern, row_start, share_rows, col_start, band_cols)
    row_global = row_start + jnp.arange(share_rows, dtype=jnp.int32)
    col_global = col_start + jnp.arange(band_cols, dtype=jnp.int32)
    identity = (row_global[:, None] == col_global[None, :]).astype(jnp.float32)
    filling = n_occ[0].astype(jnp.float32) / order
    start = mask * (
        filling * identity + gamma[0] * (mu[0] * identity - hamiltonian.astype(jnp.float32))
    )
    current = start.astype(jnp.bfloat16)
    result = start
    for iteration in range(STEPS):
        column = lax.all_gather(current, ("row", "layer"), axis=0, tiled=True)

        def rows_product(left_share):
            return jnp.dot(
                lax.all_gather(left_share, "col", axis=1, tiled=True),
                column,
                preferred_element_type=jnp.float32,
            )

        square = mask * rows_product(current)
        cube = mask * rows_product(square.astype(jnp.bfloat16))
        result = 3.0 * square - 2.0 * cube
        current = result.astype(jnp.bfloat16)
    return result


F32 = jnp.float32
BF16 = jnp.bfloat16
Z_UP, Z_DOWN, L_UP, L_DOWN, TO_Y, TO_CORE = range(6)


def kernel(sizes, cur, flags, out, full, square, half, half2, strip, column, send1, recv1, send2, recv2, send3, recv3):
    n_row, n_col, n_layer, bm, bn = sizes
    order = bn * n_col
    half_order = order // 2
    bands = n_col // 2
    row, z, layer = lax.axis_index("row"), lax.axis_index("col"), lax.axis_index("layer")
    y, core = row // 2, row % 2
    row_y = (1 - y) * 2 + core
    row_c = y * 2 + 1 - core
    row_yc = (1 - y) * 2 + 1 - core

    barrier = pltpu.get_barrier_semaphore()

    def greet(cond, device):
        @pl.when(cond)
        def _():
            pl.semaphore_signal(barrier, inc=1, device_id=device, device_id_type=pl.DeviceIdType.MESH)

    neighbours = [
        (z > 0, {"col": z - 1}),
        (z < n_col - 1, {"col": z + 1}),
        (layer > 0, {"layer": layer - 1}),
        (layer < n_layer - 1, {"layer": layer + 1}),
    ]
    for cond, device in neighbours:
        greet(cond, device)
    for device in ({"row": row_y}, {"row": row_c}):
        pl.semaphore_signal(barrier, inc=1, device_id=device, device_id_type=pl.DeviceIdType.MESH)
    peers = 2
    for cond, _device in neighbours:
        peers = peers + jnp.where(cond, 1, 0)
    pl.semaphore_wait(barrier, peers)

    def rows_of(r, l):
        return pl.ds(pl.multiple_of((r * n_layer + l) * bm, bm), bm)

    def cols_of(b):
        return pl.ds(pl.multiple_of(b * bn, bn), bn)

    def always(cond, body):
        if cond is None:
            body()
        else:
            pl.when(cond)(body)

    def both(a, b):
        if a is None:
            return b
        if b is None:
            return a
        return jnp.logical_and(a, b)

    class Gather:
        def __init__(self, view, index, send, recv):
            self.view, self.index, self.send, self.recv = view, index, send, recv
            self.pending = []

        def copy(self, way, block, device, src=None):
            dst = self.view(*block)
            at = self.index(*block)
            return pltpu.make_async_remote_copy(
                src_ref=dst if src is None else src,
                dst_ref=dst,
                send_sem=self.send.at[way, at],
                recv_sem=self.recv.at[at],
                device_id=device,
                device_id_type=pl.DeviceIdType.MESH,
            )

        def start(self, cond, way, block, device, src=None):
            always(cond, lambda: self.copy(way, block, device, src).start())
            self.pending.append((cond, way, block, device, src))

        def arrive(self, cond, block):
            always(cond, lambda: self.copy(TO_CORE, block, {"row": row_c}).wait_recv())

        def drain(self):
            for cond, way, block, device, src in self.pending:
                always(cond, lambda: self.copy(way, block, device, src).wait_send())

    g = Gather(
        lambda r, l, b: full.at[rows_of(r, l), cols_of(b)],
        lambda r, l, b: (r * n_layer + l) * n_col + b,
        send1,
        recv1,
    )

    def spread(cond, block, up, down, src=None):
        r, l, b = block
        if up:
            g.start(both(cond, layer < n_layer - 1), L_UP, block, {"layer": layer + 1}, src)
        if down:
            g.start(both(cond, layer > 0), L_DOWN, block, {"layer": layer - 1}, src)
        g.start(both(cond, b // bands == y), TO_Y, block, {"row": row_y}, src)
        g.start(cond, TO_CORE, block, {"row": row_c}, src)

    mine = (row, layer, z)
    g.start(z < n_col - 1, Z_UP, mine, {"col": z + 1}, cur)
    g.start(z > 0, Z_DOWN, mine, {"col": z - 1}, cur)
    spread(None, mine, True, True, cur)
    full[rows_of(row, layer), cols_of(z)] = cur[...]

    def layer_arrivals(cond, b):
        for e in range(1, n_layer):
            for sign in (-1, 1):
                l = layer + sign * e
                inside = both(cond, l >= 0 if sign < 0 else l < n_layer)
                g.arrive(inside, (row, l, b))
                spread(inside, (row, l, b), sign < 0, sign > 0)

    for d in range(1, n_col):
        for sign in (-1, 1):
            b = z + sign * d
            inside = b >= 0 if sign < 0 else b < n_col
            block = (row, layer, b)
            g.arrive(inside, block)
            if sign < 0:
                g.start(both(inside, z < n_col - 1), Z_UP, block, {"col": z + 1})
            else:
                g.start(both(inside, z > 0), Z_DOWN, block, {"col": z - 1})
            spread(inside, block, True, True)
        if d == 1:
            layer_arrivals(None, z)
        else:
            layer_arrivals(z - d + 1 >= 0, z - d + 1)
            layer_arrivals(z + d - 1 < n_col, z + d - 1)
    layer_arrivals(z - n_col + 1 >= 0, z - n_col + 1)
    layer_arrivals(z + n_col - 1 < n_col, z + n_col - 1)
    for b in range(bands):
        for l in range(n_layer):
            block = (row_y, l, (1 - y) * bands + b)
            g.arrive(None, block)
            g.start(None, TO_CORE, block, {"row": row_c})
    for l in range(n_layer):
        for b in range(n_col):
            g.arrive(None, (row_c, l, b))

    mine_at = pl.multiple_of(y * half_order, half_order)
    other_at = pl.multiple_of((1 - y) * half_order, half_order)

    @pl.loop(0, half_order // TILE)
    def _(t):
        here = pl.ds(pl.multiple_of(mine_at + t * TILE, TILE), TILE)
        full[pl.ds(other_at, half_order), here] = full[here, pl.ds(other_at, half_order)].T

    for l in range(n_layer):
        for b in range(bands):
            g.arrive(None, (row_yc, l, (1 - y) * bands + b))
    own_rows = rows_of(row, layer)

    def mask_of(b):
        tiles = flags.shape[1]
        tile = lax.broadcasted_iota(jnp.int32, (tiles, bn), 0)
        column_tile = (b * bn + lax.broadcasted_iota(jnp.int32, (tiles, bn), 1)) // TILE
        return jnp.dot(flags[...], (tile == column_tile).astype(BF16), preferred_element_type=F32)

    @pl.loop(0, n_col)
    def _(b):
        value = mask_of(b) * jnp.dot(full[own_rows, :], full[:, cols_of(b)], preferred_element_type=F32)
        square[:, cols_of(b)] = value
        half[:, cols_of(b)] = value.astype(BF16)

    cut = bn // 2 // TILE * TILE
    chunks = ((0, cut), (cut, bn - cut)) if cut else ((0, bn),)
    c = Gather(
        lambda r, l, h: column.at[rows_of(r, l), pl.ds(*chunks[h])],
        lambda r, l, h: (r * n_layer + l) * 2 + h,
        send2,
        recv2,
    )

    def cube_band(b):
        cube = mask_of(b) * jnp.dot(half[...], full[:, cols_of(b)], preferred_element_type=F32)
        return (3.0 * square[:, cols_of(b)] - 2.0 * cube).astype(BF16)

    def spread_column(cond, block, up, down):
        if up:
            c.start(both(cond, layer < n_layer - 1), L_UP, block, {"layer": layer + 1})
        if down:
            c.start(both(cond, layer > 0), L_DOWN, block, {"layer": layer - 1})
        c.start(cond, TO_Y, block, {"row": row_y})
        c.start(cond, TO_CORE, block, {"row": row_c})

    first = cube_band(z)
    column[own_rows, :] = first
    strip[:, cols_of(z)] = first
    for h in range(len(chunks)):
        spread_column(None, (row, layer, h), True, True)

    @pl.loop(1, n_col)
    def _(i):
        b = lax.rem(z + i, n_col)
        strip[:, cols_of(b)] = cube_band(b)

    s = Gather(
        lambda b, h: half2.at[:, pl.ds(pl.multiple_of(b * bn + chunks[h][0], TILE), chunks[h][1])],
        lambda b, h: b * 2 + h,
        send3,
        recv3,
    )
    mask_z = mask_of(z)
    for h in range(len(chunks)):
        for e in range(1, n_layer):
            for sign in (-1, 1):
                l = layer + sign * e
                inside = l >= 0 if sign < 0 else l < n_layer
                c.arrive(inside, (row, l, h))
                spread_column(inside, (row, l, h), sign < 0, sign > 0)
    for h, (at, width) in enumerate(chunks):
        for l in range(n_layer):
            c.arrive(None, (row_y, l, h))
            c.start(None, TO_CORE, (row_y, l, h), {"row": row_c})
        for l in range(n_layer):
            c.arrive(None, (row_c, l, h))
        for l in range(n_layer):
            c.arrive(None, (row_yc, l, h))
        here = slice(at, at + width)
        last = mask_z[:, here] * jnp.dot(strip[...], column[:, here], preferred_element_type=F32)
        out[:, here] = 3.0 * last
        half2[:, pl.ds(pl.multiple_of(z * bn + at, TILE), width)] = last.astype(BF16)
        s.start(z < n_col - 1, Z_UP, (z, h), {"col": z + 1})
        s.start(z > 0, Z_DOWN, (z, h), {"col": z - 1})

    def cube_part(b):
        part = jnp.dot(half2[:, cols_of(b)], column[cols_of(b), :], preferred_element_type=F32)
        out[...] -= (2.0 * mask_z) * part

    cube_part(z)
    for d in range(1, n_col):
        for sign in (-1, 1):
            b = z + sign * d
            inside = b >= 0 if sign < 0 else b < n_col
            for h in range(len(chunks)):
                s.arrive(inside, (b, h))
                if sign < 0:
                    s.start(both(inside, z < n_col - 1), Z_UP, (b, h), {"col": z + 1})
                else:
                    s.start(both(inside, z > 0), Z_DOWN, (b, h), {"col": z - 1})
        for sign in (-1, 1):
            b = z + sign * d
            inside = b >= 0 if sign < 0 else b < n_col
            always(inside, functools.partial(cube_part, b))
    s.drain()
    c.drain()
    g.drain()


def shards(hamiltonian, tile_pattern, n_occ, mu, gamma):
    bm, bn = hamiltonian.shape
    n_row, n_col, n_layer = (lax.axis_size(a) for a in ("row", "col", "layer"))
    order = bn * n_col
    vmem = 2 * order * (order + 3 * bm + bn) + 4 * bm * (order + bn) + 2 * bm * bn
    regular = n_row == 4 and n_col % 2 == 0 and n_layer * bm * n_row == order
    aligned = bm % 16 == 0 and bn % TILE == 0 and (order // 2) % TILE == 0
    if not (regular and aligned and vmem <= 48 << 20):
        return plain_shards(hamiltonian, tile_pattern, n_occ, mu, gamma)
    row_start = (lax.axis_index("row") * n_layer + lax.axis_index("layer")) * bm
    col_start = lax.axis_index("col") * bn
    rows = row_start + jnp.arange(bm, dtype=jnp.int32)
    cols = col_start + jnp.arange(bn, dtype=jnp.int32)
    tile_ids = jnp.arange(tile_pattern.shape[0], dtype=jnp.int32)
    row_hot = (rows[:, None] // TILE == tile_ids[None, :]).astype(BF16)
    flags = jnp.dot(row_hot, tile_pattern.astype(BF16), preferred_element_type=F32).astype(BF16)
    col_hot = (tile_ids[:, None] == cols[None, :] // TILE).astype(BF16)
    mask = jnp.dot(flags, col_hot, preferred_element_type=F32)
    identity = (rows[:, None] == cols[None, :]).astype(F32)
    filling = n_occ[0].astype(F32) / order
    start = mask * (filling * identity + gamma[0] * (mu[0] * identity - hamiltonian.astype(F32)))
    blocks = n_row * n_layer
    return pl.pallas_call(
        functools.partial(kernel, (n_row, n_col, n_layer, bm, bn)),
        out_shape=jax.ShapeDtypeStruct((bm, bn), F32),
        in_specs=[pl.BlockSpec(memory_space=pltpu.VMEM)] * 2,
        out_specs=pl.BlockSpec(memory_space=pltpu.VMEM),
        scratch_shapes=[
            pltpu.VMEM((order, order), BF16),
            pltpu.VMEM((bm, order), F32),
            pltpu.VMEM((bm, order), BF16),
            pltpu.VMEM((bm, order), BF16),
            pltpu.VMEM((bm, order), BF16),
            pltpu.VMEM((order, bn), BF16),
            pltpu.SemaphoreType.DMA((6, blocks * n_col)),
            pltpu.SemaphoreType.DMA((blocks * n_col,)),
            pltpu.SemaphoreType.DMA((6, blocks * 2)),
            pltpu.SemaphoreType.DMA((blocks * 2,)),
            pltpu.SemaphoreType.DMA((2, n_col * 2)),
            pltpu.SemaphoreType.DMA((n_col * 2,)),
        ],
        compiler_params=pltpu.CompilerParams(
            collective_id=0, has_side_effects=True, vmem_limit_bytes=60 << 20
        ),
    )(start.astype(BF16), flags)


def solution(mesh):
    placed = (P(("row", "layer"), "col"), P(), P(), P(), P())
    return jax.shard_map(
        shards, mesh=mesh, in_specs=placed, out_specs=P(("row", "layer"), "col"), check_vma=False
    )
```

```python
import functools

import jax
import jax.numpy as jnp
from jax import lax
from jax.experimental import pallas as pl
from jax.experimental.pallas import tpu as pltpu
from jax.sharding import PartitionSpec as P

TILE = 128
STEPS = 2


def element_mask(tile_pattern, row_start, row_count, col_start, col_count):
    tile_count = tile_pattern.shape[0]
    tile_ids = jnp.arange(tile_count, dtype=jnp.int32)
    row_tiles = (row_start + jnp.arange(row_count, dtype=jnp.int32)) // TILE
    col_tiles = (col_start + jnp.arange(col_count, dtype=jnp.int32)) // TILE
    row_hot = (row_tiles[:, None] == tile_ids[None, :]).astype(jnp.bfloat16)
    col_hot = (tile_ids[:, None] == col_tiles[None, :]).astype(jnp.bfloat16)
    picked = jnp.dot(row_hot, tile_pattern.astype(jnp.bfloat16), preferred_element_type=jnp.float32)
    return jnp.dot(picked.astype(jnp.bfloat16), col_hot, preferred_element_type=jnp.float32)


def plain_shards(hamiltonian, tile_pattern, n_occ, mu, gamma):
    share_rows, band_cols = hamiltonian.shape
    n_col = lax.axis_size("col")
    n_layer = lax.axis_size("layer")
    order = band_cols * n_col
    layer_index = lax.axis_index("layer")
    row_start = (lax.axis_index("row") * n_layer + layer_index) * share_rows
    col_start = lax.axis_index("col") * band_cols
    mask = element_mask(tile_pattern, row_start, share_rows, col_start, band_cols)
    row_global = row_start + jnp.arange(share_rows, dtype=jnp.int32)
    col_global = col_start + jnp.arange(band_cols, dtype=jnp.int32)
    identity = (row_global[:, None] == col_global[None, :]).astype(jnp.float32)
    filling = n_occ[0].astype(jnp.float32) / order
    start = mask * (
        filling * identity + gamma[0] * (mu[0] * identity - hamiltonian.astype(jnp.float32))
    )
    current = start.astype(jnp.bfloat16)
    result = start
    for iteration in range(STEPS):
        column = lax.all_gather(current, ("row", "layer"), axis=0, tiled=True)

        def rows_product(left_share):
            return jnp.dot(
                lax.all_gather(left_share, "col", axis=1, tiled=True),
                column,
                preferred_element_type=jnp.float32,
            )

        square = mask * rows_product(current)
        cube = mask * rows_product(square.astype(jnp.bfloat16))
        result = 3.0 * square - 2.0 * cube
        current = result.astype(jnp.bfloat16)
    return result


F32 = jnp.float32
BF16 = jnp.bfloat16
Z_UP, Z_DOWN, L_UP, L_DOWN, TO_Y, TO_CORE = range(6)


def kernel(sizes, cur, flags, out, full, square, half, half2, strip, column, send1, recv1, send2, recv2, send3, recv3):
    n_row, n_col, n_layer, bm, bn = sizes
    order = bn * n_col
    half_order = order // 2
    bands = n_col // 2
    row, z, layer = lax.axis_index("row"), lax.axis_index("col"), lax.axis_index("layer")
    y, core = row // 2, row % 2
    row_y = (1 - y) * 2 + core
    row_c = y * 2 + 1 - core
    row_yc = (1 - y) * 2 + 1 - core

    barrier = pltpu.get_barrier_semaphore()

    def greet(cond, device):
        @pl.when(cond)
        def _():
            pl.semaphore_signal(barrier, inc=1, device_id=device, device_id_type=pl.DeviceIdType.MESH)

    neighbours = [
        (z > 0, {"col": z - 1}),
        (z < n_col - 1, {"col": z + 1}),
        (layer > 0, {"layer": layer - 1}),
        (layer < n_layer - 1, {"layer": layer + 1}),
    ]
    for cond, device in neighbours:
        greet(cond, device)
    for device in ({"row": row_y}, {"row": row_c}):
        pl.semaphore_signal(barrier, inc=1, device_id=device, device_id_type=pl.DeviceIdType.MESH)
    peers = 2
    for cond, _device in neighbours:
        peers = peers + jnp.where(cond, 1, 0)
    pl.semaphore_wait(barrier, peers)

    def rows_of(r, l):
        return pl.ds(pl.multiple_of((r * n_layer + l) * bm, bm), bm)

    def part_of(r, l, h):
        return pl.ds(pl.multiple_of((r * n_layer + l) * bm + h * (bm // 2), bm // 2), bm // 2)

    def cols_of(b):
        return pl.ds(pl.multiple_of(b * bn, bn), bn)

    def always(cond, body):
        if cond is None:
            body()
        else:
            pl.when(cond)(body)

    def both(a, b):
        if a is None:
            return b
        if b is None:
            return a
        return jnp.logical_and(a, b)

    class Gather:
        def __init__(self, view, index, send, recv):
            self.view, self.index, self.send, self.recv = view, index, send, recv
            self.pending = []

        def copy(self, way, block, device, src=None):
            dst = self.view(*block)
            at = self.index(*block)
            return pltpu.make_async_remote_copy(
                src_ref=dst if src is None else src,
                dst_ref=dst,
                send_sem=self.send.at[way, at],
                recv_sem=self.recv.at[at],
                device_id=device,
                device_id_type=pl.DeviceIdType.MESH,
            )

        def start(self, cond, way, block, device, src=None):
            always(cond, lambda: self.copy(way, block, device, src).start())
            self.pending.append((cond, way, block, device, src))

        def arrive(self, cond, block):
            always(cond, lambda: self.copy(TO_CORE, block, {"row": row_c}).wait_recv())

        def drain(self):
            for cond, way, block, device, src in self.pending:
                always(cond, lambda: self.copy(way, block, device, src).wait_send())

    g = Gather(
        lambda r, l, b, h: full.at[part_of(r, l, h), cols_of(b)],
        lambda r, l, b, h: ((r * n_layer + l) * n_col + b) * 2 + h,
        send1,
        recv1,
    )

    def spread(cond, block, up, down, src=None):
        b = block[2]
        if up:
            g.start(both(cond, layer < n_layer - 1), L_UP, block, {"layer": layer + 1}, src)
        if down:
            g.start(both(cond, layer > 0), L_DOWN, block, {"layer": layer - 1}, src)
        g.start(both(cond, b // bands == y), TO_Y, block, {"row": row_y}, src)
        g.start(cond, TO_CORE, block, {"row": row_c}, src)

    for h in range(2):
        mine = (row, layer, z, h)
        piece = cur.at[pl.ds(h * (bm // 2), bm // 2), :]
        g.start(z < n_col - 1, Z_UP, mine, {"col": z + 1}, piece)
        g.start(z > 0, Z_DOWN, mine, {"col": z - 1}, piece)
        spread(None, mine, True, True, piece)
    full[rows_of(row, layer), cols_of(z)] = cur[...]

    def layer_arrivals(cond, b):
        for e in range(1, n_layer):
            for sign in (-1, 1):
                l = layer + sign * e
                inside = both(cond, l >= 0 if sign < 0 else l < n_layer)
                for h in range(2):
                    g.arrive(inside, (row, l, b, h))
                    spread(inside, (row, l, b, h), sign < 0, sign > 0)

    for d in range(1, n_col):
        for sign in (-1, 1):
            b = z + sign * d
            inside = b >= 0 if sign < 0 else b < n_col
            for h in range(2):
                block = (row, layer, b, h)
                g.arrive(inside, block)
                if sign < 0:
                    g.start(both(inside, z < n_col - 1), Z_UP, block, {"col": z + 1})
                else:
                    g.start(both(inside, z > 0), Z_DOWN, block, {"col": z - 1})
                spread(inside, block, True, True)
        if d == 1:
            layer_arrivals(None, z)
        else:
            layer_arrivals(z - d + 1 >= 0, z - d + 1)
            layer_arrivals(z + d - 1 < n_col, z + d - 1)
    layer_arrivals(z - n_col + 1 >= 0, z - n_col + 1)
    layer_arrivals(z + n_col - 1 < n_col, z + n_col - 1)
    for b in range(bands):
        for l in range(n_layer):
            for h in range(2):
                block = (row_y, l, (1 - y) * bands + b, h)
                g.arrive(None, block)
                g.start(None, TO_CORE, block, {"row": row_c})
    for l in range(n_layer):
        for b in range(n_col):
            for h in range(2):
                g.arrive(None, (row_c, l, b, h))

    mine_at = pl.multiple_of(y * half_order, half_order)
    other_at = pl.multiple_of((1 - y) * half_order, half_order)

    @pl.loop(0, half_order // TILE)
    def _(t):
        here = pl.ds(pl.multiple_of(mine_at + t * TILE, TILE), TILE)
        full[pl.ds(other_at, half_order), here] = full[here, pl.ds(other_at, half_order)].T

    for l in range(n_layer):
        for b in range(bands):
            for h in range(2):
                g.arrive(None, (row_yc, l, (1 - y) * bands + b, h))
    own_rows = rows_of(row, layer)

    def mask_of(b):
        tiles = flags.shape[1]
        tile = lax.broadcasted_iota(jnp.int32, (tiles, bn), 0)
        column_tile = (b * bn + lax.broadcasted_iota(jnp.int32, (tiles, bn), 1)) // TILE
        return jnp.dot(flags[...], (tile == column_tile).astype(BF16), preferred_element_type=F32)

    @pl.loop(0, n_col)
    def _(b):
        value = mask_of(b) * jnp.dot(full[own_rows, :], full[:, cols_of(b)], preferred_element_type=F32)
        square[:, cols_of(b)] = value
        half[:, cols_of(b)] = value.astype(BF16)

    cut = bn // 2 // TILE * TILE
    chunks = ((0, cut), (cut, bn - cut)) if cut else ((0, bn),)
    c = Gather(
        lambda r, l, h: column.at[rows_of(r, l), pl.ds(*chunks[h])],
        lambda r, l, h: (r * n_layer + l) * 2 + h,
        send2,
        recv2,
    )

    def cube_band(b):
        cube = mask_of(b) * jnp.dot(half[...], full[:, cols_of(b)], preferred_element_type=F32)
        return (3.0 * square[:, cols_of(b)] - 2.0 * cube).astype(BF16)

    def spread_column(cond, block, up, down):
        if up:
            c.start(both(cond, layer < n_layer - 1), L_UP, block, {"layer": layer + 1})
        if down:
            c.start(both(cond, layer > 0), L_DOWN, block, {"layer": layer - 1})
        c.start(cond, TO_Y, block, {"row": row_y})
        c.start(cond, TO_CORE, block, {"row": row_c})

    first = cube_band(z)
    column[own_rows, :] = first
    strip[:, cols_of(z)] = first
    for h in range(len(chunks)):
        spread_column(None, (row, layer, h), True, True)

    @pl.loop(1, n_col)
    def _(i):
        b = lax.rem(z + i, n_col)
        strip[:, cols_of(b)] = cube_band(b)

    s = Gather(
        lambda b, h: half2.at[:, pl.ds(pl.multiple_of(b * bn + chunks[h][0], TILE), chunks[h][1])],
        lambda b, h: b * 2 + h,
        send3,
        recv3,
    )
    mask_z = mask_of(z)
    for h in range(len(chunks)):
        for e in range(1, n_layer):
            for sign in (-1, 1):
                l = layer + sign * e
                inside = l >= 0 if sign < 0 else l < n_layer
                c.arrive(inside, (row, l, h))
                spread_column(inside, (row, l, h), sign < 0, sign > 0)
    for h, (at, width) in enumerate(chunks):
        for l in range(n_layer):
            c.arrive(None, (row_y, l, h))
            c.start(None, TO_CORE, (row_y, l, h), {"row": row_c})
        for l in range(n_layer):
            c.arrive(None, (row_c, l, h))
        for l in range(n_layer):
            c.arrive(None, (row_yc, l, h))
        here = slice(at, at + width)
        last = mask_z[:, here] * jnp.dot(strip[...], column[:, here], preferred_element_type=F32)
        out[:, here] = 3.0 * last
        half2[:, pl.ds(pl.multiple_of(z * bn + at, TILE), width)] = last.astype(BF16)
        s.start(z < n_col - 1, Z_UP, (z, h), {"col": z + 1})
        s.start(z > 0, Z_DOWN, (z, h), {"col": z - 1})

    def cube_part(b):
        part = jnp.dot(half2[:, cols_of(b)], column[cols_of(b), :], preferred_element_type=F32)
        out[...] -= (2.0 * mask_z) * part

    cube_part(z)
    for d in range(1, n_col):
        for sign in (-1, 1):
            b = z + sign * d
            inside = b >= 0 if sign < 0 else b < n_col
            for h in range(len(chunks)):
                s.arrive(inside, (b, h))
                if sign < 0:
                    s.start(both(inside, z < n_col - 1), Z_UP, (b, h), {"col": z + 1})
                else:
                    s.start(both(inside, z > 0), Z_DOWN, (b, h), {"col": z - 1})
        for sign in (-1, 1):
            b = z + sign * d
            inside = b >= 0 if sign < 0 else b < n_col
            always(inside, functools.partial(cube_part, b))
    s.drain()
    c.drain()
    g.drain()


def shards(hamiltonian, tile_pattern, n_occ, mu, gamma):
    bm, bn = hamiltonian.shape
    n_row, n_col, n_layer = (lax.axis_size(a) for a in ("row", "col", "layer"))
    order = bn * n_col
    vmem = 2 * order * (order + 3 * bm + bn) + 4 * bm * (order + bn) + 2 * bm * bn
    regular = n_row == 4 and n_col % 2 == 0 and n_layer * bm * n_row == order
    aligned = bm % 32 == 0 and bn % TILE == 0 and (order // 2) % TILE == 0
    if not (regular and aligned and vmem <= 48 << 20):
        return plain_shards(hamiltonian, tile_pattern, n_occ, mu, gamma)
    row_start = (lax.axis_index("row") * n_layer + lax.axis_index("layer")) * bm
    col_start = lax.axis_index("col") * bn
    rows = row_start + jnp.arange(bm, dtype=jnp.int32)
    cols = col_start + jnp.arange(bn, dtype=jnp.int32)
    tile_ids = jnp.arange(tile_pattern.shape[0], dtype=jnp.int32)
    row_hot = (rows[:, None] // TILE == tile_ids[None, :]).astype(BF16)
    flags = jnp.dot(row_hot, tile_pattern.astype(BF16), preferred_element_type=F32).astype(BF16)
    col_hot = (tile_ids[:, None] == cols[None, :] // TILE).astype(BF16)
    mask = jnp.dot(flags, col_hot, preferred_element_type=F32)
    identity = (rows[:, None] == cols[None, :]).astype(F32)
    filling = n_occ[0].astype(F32) / order
    start = mask * (filling * identity + gamma[0] * (mu[0] * identity - hamiltonian.astype(F32)))
    blocks = n_row * n_layer
    return pl.pallas_call(
        functools.partial(kernel, (n_row, n_col, n_layer, bm, bn)),
        out_shape=jax.ShapeDtypeStruct((bm, bn), F32),
        in_specs=[pl.BlockSpec(memory_space=pltpu.VMEM)] * 2,
        out_specs=pl.BlockSpec(memory_space=pltpu.VMEM),
        scratch_shapes=[
            pltpu.VMEM((order, order), BF16),
            pltpu.VMEM((bm, order), F32),
            pltpu.VMEM((bm, order), BF16),
            pltpu.VMEM((bm, order), BF16),
            pltpu.VMEM((bm, order), BF16),
            pltpu.VMEM((order, bn), BF16),
            pltpu.SemaphoreType.DMA((6, blocks * n_col * 2)),
            pltpu.SemaphoreType.DMA((blocks * n_col * 2,)),
            pltpu.SemaphoreType.DMA((6, blocks * 2)),
            pltpu.SemaphoreType.DMA((blocks * 2,)),
            pltpu.SemaphoreType.DMA((2, n_col * 2)),
            pltpu.SemaphoreType.DMA((n_col * 2,)),
        ],
        compiler_params=pltpu.CompilerParams(
            collective_id=0, has_side_effects=True, vmem_limit_bytes=60 << 20
        ),
    )(start.astype(BF16), flags)


def solution(mesh):
    placed = (P(("row", "layer"), "col"), P(), P(), P(), P())
    return jax.shard_map(
        shards, mesh=mesh, in_specs=placed, out_specs=P(("row", "layer"), "col"), check_vma=False
    )
```
